32 devices in a mesh: ka: 16 (over z, x, core), pa: 2 (over y).
Axes of the slice: x: 2, y: 2, z: 4, core: 2. Of those that a mesh axis runs over, the one named last changes fastest.
Arguments:
- pairs: bfloat16 [64, 64, 2048], P('pa', 'ka'), may hold values from -6 to 6
- eps_val: float32 [64, 64], P('ka'), may hold values from -1.5 to -0.2
- eps_cond: float32 [64, 64], P('ka'), may hold values from 0.2 to 1.5
- orb_val: bfloat16 [64, 64, 12288], P('ka', None, 'pa'), may hold values from -0.625 to 0.625
- orb_cond: bfloat16 [64, 64, 12288], P('ka', None, 'pa'), may hold values from -0.625 to 0.625
- screened: bfloat16 [12288, 12288], P('ka', 'pa'), may hold values from -0.25 to 0.25
Outputs:
- applied: bfloat16 [64, 64, 2048], P('pa', 'ka')
The draws below stay inside these ranges and needn't reach their ends.
All inputs are finite; a program needn't handle non-finite values.
Results may differ from the reference program's by a relative error of at most 0.0055.
Values may be sent and summed in bfloat16 or wider, within the bound.
A program may use at most 64 MiB of HBM per device.

```python
import jax
import jax.numpy as jnp
from jax import lax

NV = 64
NC = 64
NMU = 12288
NB = 32
K = 64


def shard_levels(own_key, extent, shards, smallest, top_value):
    loudness = 1.0
    for axis_at, parts in shards:
        draws = jax.random.uniform(jax.random.fold_in(jax.random.fold_in(own_key, 6), axis_at), (parts,), jnp.float32, smallest / len(shards), top_value / len(shards))
        loudness = loudness * jnp.repeat(jnp.exp(draws), extent[axis_at] // parts).reshape((-1,) + (1,) * (len(extent) - 1 - axis_at))
    return loudness


def normal_values(stream_key, shape, spread, most, cuts=(), dtype=jnp.bfloat16):
    entries = spread * jax.random.normal(stream_key, shape, jnp.float32)
    if cuts:
        entries = entries * shard_levels(stream_key, shape, cuts, -0.22, 0.18)
    return jnp.clip(entries, -most, most).astype(dtype)


def setup_inputs(seed: int = 0) -> dict:
    splits = jax.random.split(jax.random.key(seed), 7)
    return {
        "pairs": normal_values(splits[0], (NV, K, NB * NC), 1.0, 6.0, ((0, 2), (1, 16))),
        "eps_val": jnp.clip(-1.5 + 1.3 * jax.random.uniform(splits[1], (K, NV), jnp.float32) ** shard_levels(splits[1], (K, NV), ((0, 16),), -0.2, 0.2), -1.5, -0.2),
        "eps_cond": jnp.clip(0.2 + 1.3 * jax.random.uniform(splits[2], (K, NC), jnp.float32) ** shard_levels(splits[2], (K, NC), ((0, 16),), -0.2, 0.2), 0.2, 1.5),
        "orb_val": normal_values(splits[3], (K, NV, NMU), ((K * NV * NC) ** -0.25), 0.625, ((0, 16), (2, 2))),
        "orb_cond": normal_values(splits[4], (K, NC, NMU), ((K * NV * NC) ** -0.25), 0.625, ((0, 16), (2, 2))),
        "screened": normal_values(splits[5], (NMU, NMU), (2.0 * NMU ** -0.5), 0.25, ((0, 16), (1, 2))),
    }


def reference(pairs, eps_val, eps_cond, orb_val, orb_cond, screened):
    highest = lax.Precision.HIGHEST
    by_kpoint = jnp.swapaxes(pairs, 0, 1)

    def forward_step(running, slices):
        pairs_here, valence, conduction = slices
        coeffs = pairs_here.astype(jnp.float32).reshape(NV, NB, NC)
        inner = jnp.einsum('vbc,cm->vbm', coeffs, conduction.astype(jnp.float32), precision=highest)
        added = jnp.einsum('vbm,vm->bm', inner, valence.astype(jnp.float32), precision=highest)
        return running + added, None

    points, _ = lax.scan(forward_step, jnp.zeros((NB, NMU), jnp.float32), (by_kpoint, orb_val, orb_cond))
    points_bf = points.astype(jnp.bfloat16)
    image = lax.dot_general(points_bf, screened, (((1,), (1,)), ((), ())), preferred_element_type=jnp.float32)
    image_bf = lax.optimization_barrier(image.astype(jnp.bfloat16))
    image_wide = image_bf.astype(jnp.float32)

    def backward_step(carry_unused, slices):
        pairs_here, valence, conduction, energy_val, energy_cond = slices
        weighted = (valence.astype(jnp.float32)[:, None, :] * image_wide[None]).astype(jnp.bfloat16)
        weighted = lax.optimization_barrier(weighted)
        coupling = jnp.einsum('vbm,cm->vbc', weighted.astype(jnp.float32), conduction.astype(jnp.float32), precision=highest)
        energy_gap = energy_cond[None, None, :] - energy_val[:, None, None]
        coeffs = pairs_here.astype(jnp.float32).reshape(NV, NB, NC)
        result = (energy_gap * coeffs + coupling).reshape(NV, NB * NC).astype(jnp.bfloat16)
        return carry_unused, result

    _, applied = lax.scan(backward_step, jnp.zeros((), jnp.float32), (by_kpoint, orb_val, orb_cond, eps_val, eps_cond))
    return jnp.swapaxes(applied, 0, 1)
```

```python
import functools

import jax
import jax.numpy as jnp
from jax import lax
from jax.experimental import pallas as pl
from jax.experimental.pallas import tpu as pltpu
from jax.sharding import PartitionSpec as P

VMEM_BYTES = 58 * 1024 * 1024


def pick_tile(extent, most):
    tile = most
    while extent % tile:
        tile //= 2
    return tile


def forward_kernel(vectors, pairs_ref, val_ref, cond_ref, out_ref, turned):
    kpoints, conds = cond_ref.shape[0], cond_ref.shape[1]
    tile = cond_ref.shape[2]

    @pl.when(pl.program_id(0) == 0)
    def _():
        for k in range(kpoints):
            turned[k] = pairs_ref[k].T

    group = 4
    wide = [cond_ref[k].astype(jnp.float32).reshape(conds // 8, 8, tile) for k in range(kpoints)]
    for g in range(vectors // group):
        total = None
        for k in range(kpoints):
            rows = turned[k, g * group * conds : (g + 1) * group * conds, :]
            inner = jnp.dot(rows, val_ref[k], preferred_element_type=jnp.float32)
            inner = inner.reshape(group, conds // 8, 8, tile)
            added = jnp.sum(inner * wide[k][None], axis=1)
            total = added if total is None else total + added
        out_ref[g * group : (g + 1) * group, :] = jnp.sum(total, axis=1)


def forward(rows, orb_val, orb_cond):
    kpoints, all_val, points_dev = orb_val.shape
    conds = orb_cond.shape[1]
    width = rows.shape[2]
    vectors = width // conds
    tile = pick_tile(points_dev, 256)
    return pl.pallas_call(
        functools.partial(forward_kernel, vectors),
        grid=(points_dev // tile,),
        out_shape=jax.ShapeDtypeStruct((vectors, points_dev), jnp.float32),
        in_specs=[
            pl.BlockSpec((kpoints, all_val, width), lambda i: (0, 0, 0)),
            pl.BlockSpec((kpoints, all_val, tile), lambda i: (0, 0, i)),
            pl.BlockSpec((kpoints, conds, tile), lambda i: (0, 0, i)),
        ],
        out_specs=pl.BlockSpec((vectors, tile), lambda i: (0, i)),
        scratch_shapes=[pltpu.VMEM((kpoints, width, all_val), jnp.bfloat16)],
        compiler_params=pltpu.CompilerParams(vmem_limit_bytes=VMEM_BYTES),
    )(rows, orb_val, orb_cond)


def backward_kernel(image_ref, val_ref, cond_ref, out_ref, total):
    vectors, tile = image_ref.shape
    conds = cond_ref.shape[1]
    group = 4
    step = pl.program_id(1)

    @pl.when(step == 0)
    def _():
        total[...] = jnp.zeros_like(total)

    valence = val_ref[0]
    conduction = cond_ref[0]
    for g in range(vectors // group):
        pieces = [
            jnp.broadcast_to(image_ref[b : b + 1, :], (conds, tile)) * conduction
            for b in range(g * group, (g + 1) * group)
        ]
        mixed = jnp.concatenate(pieces, axis=0)
        cols = slice(g * group * conds, (g + 1) * group * conds)
        total[:, cols] += lax.dot_general(
            valence, mixed, (((1,), (1,)), ((), ())), preferred_element_type=jnp.float32
        )

    @pl.when(step == pl.num_programs(1) - 1)
    def _():
        out_ref[0] = total[...].astype(out_ref.dtype)


def backward(image, orb_val, orb_cond):
    kpoints, all_val, points_dev = orb_val.shape
    conds = orb_cond.shape[1]
    vectors = image.shape[0]
    tile = pick_tile(points_dev, 1024)
    return pl.pallas_call(
        backward_kernel,
        grid=(kpoints, points_dev // tile),
        out_shape=jax.ShapeDtypeStruct((kpoints, all_val, vectors * conds), jnp.bfloat16),
        in_specs=[
            pl.BlockSpec((vectors, tile), lambda k, i: (0, i)),
            pl.BlockSpec((1, all_val, tile), lambda k, i: (k, 0, i)),
            pl.BlockSpec((1, conds, tile), lambda k, i: (k, 0, i)),
        ],
        out_specs=pl.BlockSpec((1, all_val, vectors * conds), lambda k, i: (k, 0, 0)),
        scratch_shapes=[pltpu.VMEM((all_val, vectors * conds), jnp.float32)],
        compiler_params=pltpu.CompilerParams(vmem_limit_bytes=VMEM_BYTES),
    )(image, orb_val, orb_cond)


def body(pairs, eps_val, eps_cond, orb_val, orb_cond, screened):
    val_rows, kpoints, width = pairs.shape
    conds = orb_cond.shape[1]
    points_dev = orb_val.shape[2]
    vectors = width // conds
    own = jnp.transpose(pairs, (1, 0, 2))
    rows = lax.all_gather(own, "pa", axis=1, tiled=True)
    partial_points = forward(rows, orb_val, orb_cond)
    points = lax.psum_scatter(partial_points, "ka", scatter_dimension=1, tiled=True)
    points_bf = lax.all_gather(points.astype(jnp.bfloat16), "ka", axis=1, tiled=True)
    image_part = lax.dot_general(
        points_bf, screened, (((1,), (1,)), ((), ())), preferred_element_type=jnp.float32
    )
    image_rows = lax.psum(image_part.astype(jnp.bfloat16), "pa")
    image_whole = lax.all_gather(image_rows, "ka", axis=1, tiled=True)
    image_block = lax.dynamic_slice_in_dim(
        image_whole, lax.axis_index("pa") * points_dev, points_dev, 1
    )
    results = backward(image_block, orb_val, orb_cond)
    coupling = lax.psum_scatter(results, "pa", scatter_dimension=1, tiled=True)
    coupling = jnp.transpose(coupling.astype(jnp.float32), (1, 0, 2))
    own_val = lax.dynamic_slice_in_dim(eps_val, lax.axis_index("pa") * val_rows, val_rows, 1)
    energy_gap = eps_cond[None, :, None, :] - jnp.transpose(own_val)[:, :, None, None]
    coeffs = pairs.astype(jnp.float32).reshape(val_rows, kpoints, vectors, conds)
    diagonal_part = (energy_gap * coeffs).reshape(val_rows, kpoints, vectors * conds)
    return (diagonal_part + coupling).astype(jnp.bfloat16)


def solution(mesh):
    in_specs = (
        P("pa", "ka", None),
        P("ka", None),
        P("ka", None),
        P("ka", None, "pa"),
        P("ka", None, "pa"),
        P("ka", "pa"),
    )
    out_specs = P("pa", "ka", None)
    return jax.shard_map(body, mesh=mesh, in_specs=in_specs, out_specs=out_specs, check_vma=False)
```

```python
import functools

import jax
import jax.numpy as jnp
from jax import lax
from jax.experimental import pallas as pl
from jax.experimental.pallas import tpu as pltpu
from jax.sharding import PartitionSpec as P

VMEM_BYTES = 58 * 1024 * 1024


def pick_tile(extent, most):
    tile = most
    while extent % tile:
        tile //= 2
    return tile


def forward_kernel(vectors, pairs_ref, val_ref, cond_ref, out_ref, turned):
    kpoints, conds = cond_ref.shape[0], cond_ref.shape[1]
    tile = cond_ref.shape[2]

    @pl.when(pl.program_id(0) == 0)
    def _():
        for k in range(kpoints):
            turned[k] = pairs_ref[k].T

    group = 4
    wide = [cond_ref[k].astype(jnp.float32).reshape(conds // 8, 8, tile) for k in range(kpoints)]
    for g in range(vectors // group):
        total = None
        for k in range(kpoints):
            rows = turned[k, g * group * conds : (g + 1) * group * conds, :]
            inner = jnp.dot(rows, val_ref[k], preferred_element_type=jnp.float32)
            inner = inner.reshape(group, conds // 8, 8, tile)
            added = jnp.sum(inner * wide[k][None], axis=1)
            total = added if total is None else total + added
        out_ref[g * group : (g + 1) * group, :] = jnp.sum(total, axis=1)


def forward(rows, orb_val, orb_cond):
    kpoints, all_val, points_dev = orb_val.shape
    conds = orb_cond.shape[1]
    width = rows.shape[2]
    vectors = width // conds
    tile = pick_tile(points_dev, 256)
    return pl.pallas_call(
        functools.partial(forward_kernel, vectors),
        grid=(points_dev // tile,),
        out_shape=jax.ShapeDtypeStruct((vectors, points_dev), jnp.float32),
        in_specs=[
            pl.BlockSpec((kpoints, all_val, width), lambda i: (0, 0, 0)),
            pl.BlockSpec((kpoints, all_val, tile), lambda i: (0, 0, i)),
            pl.BlockSpec((kpoints, conds, tile), lambda i: (0, 0, i)),
        ],
        out_specs=pl.BlockSpec((vectors, tile), lambda i: (0, i)),
        scratch_shapes=[pltpu.VMEM((kpoints, width, all_val), jnp.bfloat16)],
        compiler_params=pltpu.CompilerParams(vmem_limit_bytes=VMEM_BYTES),
    )(rows, orb_val, orb_cond)


def backward_kernel(image_ref, val_ref, cond_ref, out_ref, total):
    vectors, tile = image_ref.shape
    conds = cond_ref.shape[1]
    group = 4
    step = pl.program_id(1)

    @pl.when(step == 0)
    def _():
        total[...] = jnp.zeros_like(total)

    valence = val_ref[0]
    conduction = cond_ref[0]
    for g in range(vectors // group):
        pieces = [
            jnp.broadcast_to(image_ref[b : b + 1, :], (conds, tile)) * conduction
            for b in range(g * group, (g + 1) * group)
        ]
        mixed = jnp.concatenate(pieces, axis=0)
        cols = slice(g * group * conds, (g + 1) * group * conds)
        total[:, cols] += lax.dot_general(
            valence, mixed, (((1,), (1,)), ((), ())), preferred_element_type=jnp.float32
        )

    @pl.when(step == pl.num_programs(1) - 1)
    def _():
        out_ref[0] = total[...].astype(out_ref.dtype)


def backward(image, orb_val, orb_cond):
    kpoints, all_val, points_dev = orb_val.shape
    conds = orb_cond.shape[1]
    vectors = image.shape[0]
    tile = pick_tile(points_dev, 1024)
    return pl.pallas_call(
        backward_kernel,
        grid=(kpoints, points_dev // tile),
        out_shape=jax.ShapeDtypeStruct((kpoints, all_val, vectors * conds), jnp.bfloat16),
        in_specs=[
            pl.BlockSpec((vectors, tile), lambda k, i: (0, i)),
            pl.BlockSpec((1, all_val, tile), lambda k, i: (k, 0, i)),
            pl.BlockSpec((1, conds, tile), lambda k, i: (k, 0, i)),
        ],
        out_specs=pl.BlockSpec((1, all_val, vectors * conds), lambda k, i: (k, 0, 0)),
        scratch_shapes=[pltpu.VMEM((all_val, vectors * conds), jnp.float32)],
        compiler_params=pltpu.CompilerParams(vmem_limit_bytes=VMEM_BYTES),
    )(image, orb_val, orb_cond)


def body_plain(pairs, eps_val, eps_cond, orb_val, orb_cond, screened):
    val_rows, kpoints, width = pairs.shape
    conds = orb_cond.shape[1]
    points_dev = orb_val.shape[2]
    vectors = width // conds
    own = jnp.transpose(pairs, (1, 0, 2))
    rows = lax.all_gather(own, "pa", axis=1, tiled=True)
    partial_points = forward(rows, orb_val, orb_cond)
    points = lax.psum_scatter(partial_points, "ka", scatter_dimension=1, tiled=True)
    points_bf = lax.all_gather(points.astype(jnp.bfloat16), "ka", axis=1, tiled=True)
    image_part = lax.dot_general(
        points_bf, screened, (((1,), (1,)), ((), ())), preferred_element_type=jnp.float32
    )
    image_rows = lax.psum(image_part.astype(jnp.bfloat16), "pa")
    image_whole = lax.all_gather(image_rows, "ka", axis=1, tiled=True)
    image_block = lax.dynamic_slice_in_dim(
        image_whole, lax.axis_index("pa") * points_dev, points_dev, 1
    )
    results = backward(image_block, orb_val, orb_cond)
    coupling = lax.psum_scatter(results, "pa", scatter_dimension=1, tiled=True)
    coupling = jnp.transpose(coupling.astype(jnp.float32), (1, 0, 2))
    own_val = lax.dynamic_slice_in_dim(eps_val, lax.axis_index("pa") * val_rows, val_rows, 1)
    energy_gap = eps_cond[None, :, None, :] - jnp.transpose(own_val)[:, :, None, None]
    coeffs = pairs.astype(jnp.float32).reshape(val_rows, kpoints, vectors, conds)
    diagonal_part = (energy_gap * coeffs).reshape(val_rows, kpoints, vectors * conds)
    return (diagonal_part + coupling).astype(jnp.bfloat16)


MESH = pl.DeviceIdType.MESH
QUARTER = 8


def forward_pair_kernel(vectors, own_ref, val_ref, cond_ref, out_ref, full, turned, early, local_sem, send_sem, recv_sem):
    kpoints, conds, tile = cond_ref.shape
    row, me = lax.axis_index("ka"), lax.axis_index("pa")
    other = 1 - me
    phase, step = pl.program_id(0), pl.program_id(1)

    def remote(k):
        return pltpu.make_async_remote_copy(
            src_ref=own_ref.at[k],
            dst_ref=full.at[me, k],
            send_sem=send_sem.at[k],
            recv_sem=recv_sem.at[k],
            device_id=(row, other),
            device_id_type=MESH,
        )

    def turn(k):
        remote(k).wait()
        turned[k] = jnp.concatenate([full[0, k], full[1, k]], axis=0).T

    @pl.when(jnp.logical_and(phase == 0, step == 0))
    def _():
        local = pltpu.make_async_copy(own_ref, full.at[me], local_sem)
        local.start()
        barrier = pltpu.get_barrier_semaphore()
        pl.semaphore_signal(barrier, inc=1, device_id=(row, other), device_id_type=MESH)
        pl.semaphore_wait(barrier, 1)
        for k in range(kpoints):
            remote(k).start()
        local.wait()
        turn(0)

    @pl.when(jnp.logical_and(phase == 1, step == 0))
    def _():
        for k in range(1, kpoints):
            turn(k)

    group = 4

    def contract(ks, g):
        total = None
        for k in ks:
            wide = cond_ref[k].astype(jnp.float32).reshape(conds // 8, 8, tile)
            rows = turned[k, g * group * conds : (g + 1) * group * conds, :]
            inner = jnp.dot(rows, val_ref[k], preferred_element_type=jnp.float32)
            inner = inner.reshape(group, conds // 8, 8, tile)
            added = jnp.sum(inner * wide[None], axis=1)
            total = added if total is None else total + added
        return jnp.sum(total, axis=1)

    @pl.when(phase == 0)
    def _():
        for g in range(vectors // group):
            early[step, g * group : (g + 1) * group, :] = contract([0], g)

    @pl.when(phase == 1)
    def _():
        parts = [contract(range(1, kpoints), g) for g in range(vectors // group)]
        out_ref[...] = (jnp.concatenate(parts, axis=0) + early[step]).astype(out_ref.dtype)


def forward_pair(own, orb_val, orb_cond):
    kpoints, all_val, points_dev = orb_val.shape
    conds = orb_cond.shape[1]
    val_rows, width = own.shape[1:]
    vectors = width // conds
    tile = 256
    return pl.pallas_call(
        functools.partial(forward_pair_kernel, vectors),
        grid=(2, points_dev // tile),
        out_shape=jax.ShapeDtypeStruct((vectors, points_dev), jnp.bfloat16),
        in_specs=[
            pl.BlockSpec(memory_space=pl.ANY),
            pl.BlockSpec((kpoints, all_val, tile), lambda h, i: (0, 0, i)),
            pl.BlockSpec((kpoints, conds, tile), lambda h, i: (0, 0, i)),
        ],
        out_specs=pl.BlockSpec((vectors, tile), lambda h, i: (0, h * i)),
        scratch_shapes=[
            pltpu.VMEM((2, kpoints, val_rows, width), jnp.bfloat16),
            pltpu.VMEM((kpoints, width, all_val), jnp.bfloat16),
            pltpu.VMEM((points_dev // tile, vectors, tile), jnp.float32),
            pltpu.SemaphoreType.DMA,
            pltpu.SemaphoreType.DMA((kpoints,)),
            pltpu.SemaphoreType.DMA((kpoints,)),
        ],
        compiler_params=pltpu.CompilerParams(
            vmem_limit_bytes=VMEM_BYTES, collective_id=0, has_side_effects=True
        ),
    )(own, orb_val, orb_cond)


def middle_kernel(
    count, part_ref, screened_ref, out_ref, near, landed, points, piece, summed, images,
    near_sem, sum_send, sum_recv, pts_send, pts_recv, mix_send, mix_recv, img_send, img_recv,
):
    me, plane = lax.axis_index("ka"), lax.axis_index("pa")
    share = landed.shape[2]
    rows_dev = near.shape[0]
    vectors = points.shape[0]
    quarters = vectors // QUARTER
    ring = count // quarters
    layers = quarters // 2

    def cols(j, size):
        return pl.ds(pl.multiple_of(j * size, 128), size)

    load = pltpu.make_async_copy(screened_ref, near, near_sem)
    load.start()

    barrier = pltpu.get_barrier_semaphore()
    for s in range(1, 2 * count):
        there = lax.rem(me * 2 + plane + s, 2 * count)
        pl.semaphore_signal(
            barrier, inc=1, device_id=(there // 2, lax.rem(there, 2)), device_id_type=MESH
        )
    pl.semaphore_wait(barrier, 2 * count - 1)

    def send_part(j, slot):
        return pltpu.make_async_remote_copy(
            src_ref=part_ref.at[:, cols(j, share)],
            dst_ref=landed.at[slot],
            send_sem=sum_send.at[j],
            recv_sem=sum_recv.at[slot],
            device_id=(j, plane),
            device_id_type=MESH,
        )

    def send_points(j, owner):
        return pltpu.make_async_remote_copy(
            src_ref=points.at[:, cols(owner, share)],
            dst_ref=points.at[:, cols(owner, share)],
            send_sem=pts_send.at[j],
            recv_sem=pts_recv.at[owner],
            device_id=(j, plane),
            device_id_type=MESH,
        )

    def send_images(j, owner):
        return pltpu.make_async_remote_copy(
            src_ref=images.at[owner],
            dst_ref=images.at[owner],
            send_sem=img_send.at[j],
            recv_sem=img_recv.at[owner],
            device_id=(j, plane),
            device_id_type=MESH,
        )

    ahead = [lax.rem(me + s, count) for s in range(1, count)]
    behind = [lax.rem(me + count - s, count) for s in range(1, count)]

    for j in ahead:
        send_part(j, me).start()
    total = part_ref[:, cols(me, share)].astype(jnp.float32)
    for j in behind:
        send_part(j, j).wait_recv()
        total = total + landed[j].astype(jnp.float32)
    points[:, cols(me, share)] = total.astype(jnp.bfloat16)
    for j in ahead:
        send_points(j, me).start()

    load.wait()
    image = None
    for s in range(count // 2):
        t = lax.rem(me // 2 + count // 2 - s, count // 2)
        if s == 0:
            send_points(t * 2 + 1 - lax.rem(me, 2), t * 2 + 1 - lax.rem(me, 2)).wait_recv()
        else:
            send_points(t * 2, t * 2).wait_recv()
            send_points(t * 2 + 1, t * 2 + 1).wait_recv()
        added = lax.dot_general(
            points[:, cols(t, 2 * share)],
            near[:, cols(t, 2 * share)],
            (((1,), (1,)), ((), ())),
            preferred_element_type=jnp.float32,
        )
        image = added if image is None else image + added
    for t in range(quarters):
        piece[t] = image[t * QUARTER : (t + 1) * QUARTER, :]

    z, r = me // ring, lax.rem(me, ring)
    target, layer = z // layers, lax.rem(z, layers)

    def send_piece(t, source_plane, source_layer):
        return pltpu.make_async_remote_copy(
            src_ref=piece.at[t],
            dst_ref=summed.at[source_plane, source_layer],
            send_sem=mix_send.at[t],
            recv_sem=mix_recv.at[source_plane * layers + source_layer],
            device_id=(t * ring + r, target),
            device_id_type=MESH,
        )

    for t in range(quarters):
        here = jnp.logical_and(target == plane, z == t)

        @pl.when(jnp.logical_not(here))
        def _():
            send_piece(t, plane, layer).start()

        @pl.when(here)
        def _():
            summed[plane, layer] = piece[t]

    for p in range(2):
        for h in range(layers):
            here = jnp.logical_and(p == plane, z == plane * layers + h)

            @pl.when(jnp.logical_not(here))
            def _():
                send_piece(0, p, h).wait_recv()

    for h in range(layers):
        images[me, :, h * rows_dev : (h + 1) * rows_dev] = (summed[0, h] + summed[1, h]).astype(
            jnp.bfloat16
        )
    for j in ahead:
        send_images(j, me).start()
    for j in ahead:
        send_part(j, me).wait_send()
        send_points(j, me).wait_send()
    for t in range(quarters):
        here = jnp.logical_and(target == plane, z == t)

        @pl.when(jnp.logical_not(here))
        def _():
            send_piece(t, plane, layer).wait_send()

    for j in behind:
        send_images(j, j).wait_recv()
    for f in range(quarters // 2):
        for c in range(ring):
            both = jnp.concatenate(
                [images[(2 * f + e) * ring + c].astype(jnp.float32) for e in range(2)], axis=0
            ).astype(jnp.bfloat16)
            for h in range(layers):
                at = (h * ring + c) * rows_dev
                out_ref[f * 2 * QUARTER : (f + 1) * 2 * QUARTER, at : at + rows_dev] = both[
                    :, h * rows_dev : (h + 1) * rows_dev
                ]
    for j in ahead:
        send_images(j, me).wait_send()


def middle(count, part, screened):
    vectors, points_dev = part.shape
    rows_dev = screened.shape[0]
    share = points_dev // count
    layers = vectors // QUARTER // 2
    dma = pltpu.SemaphoreType.DMA
    return pl.pallas_call(
        functools.partial(middle_kernel, count),
        out_shape=jax.ShapeDtypeStruct((vectors, points_dev), jnp.bfloat16),
        in_specs=[pl.BlockSpec(memory_space=pltpu.VMEM), pl.BlockSpec(memory_space=pl.ANY)],
        out_specs=pl.BlockSpec(memory_space=pltpu.VMEM),
        scratch_shapes=[
            pltpu.VMEM((rows_dev, points_dev), jnp.bfloat16),
            pltpu.VMEM((count, vectors, share), jnp.bfloat16),
            pltpu.VMEM((vectors, points_dev), jnp.bfloat16),
            pltpu.VMEM((vectors // QUARTER, QUARTER, rows_dev), jnp.float32),
            pltpu.VMEM((2, layers, QUARTER, rows_dev), jnp.float32),
            pltpu.VMEM((count, QUARTER, layers * rows_dev), jnp.bfloat16),
            dma,
            dma((count,)),
            dma((count,)),
            dma((count,)),
            dma((count,)),
            dma((vectors // QUARTER,)),
            dma((2 * layers,)),
            dma((count,)),
            dma((count,)),
        ],
        compiler_params=pltpu.CompilerParams(
            vmem_limit_bytes=VMEM_BYTES, collective_id=1, has_side_effects=True
        ),
    )(part, screened)


def backward_pair_kernel(
    image_ref, val_ref, cond_ref, own_ref, level_val_ref, level_cond_ref, out_ref,
    total, kept, away, landed, send_sem, recv_sem,
):
    vectors, tile = image_ref.shape
    conds = cond_ref.shape[1]
    kpoints, val_rows = own_ref.shape[:2]
    group = 4
    at, step = pl.program_id(0), pl.program_id(1)
    row, me = lax.axis_index("ka"), lax.axis_index("pa")
    other = 1 - me

    def remote(k):
        return pltpu.make_async_remote_copy(
            src_ref=away.at[k],
            dst_ref=landed.at[k],
            send_sem=send_sem.at[k],
            recv_sem=recv_sem.at[k],
            device_id=(row, other),
            device_id_type=MESH,
        )

    @pl.when(jnp.logical_and(at == 0, step == 0))
    def _():
        barrier = pltpu.get_barrier_semaphore()
        pl.semaphore_signal(barrier, inc=1, device_id=(row, other), device_id_type=MESH)
        pl.semaphore_wait(barrier, 1)

    @pl.when(step == 0)
    def _():
        total[...] = jnp.zeros_like(total)

    valence = val_ref[0]
    conduction = cond_ref[0]
    for g in range(vectors // group):
        pieces = [
            jnp.broadcast_to(image_ref[b : b + 1, :], (conds, tile)) * conduction
            for b in range(g * group, (g + 1) * group)
        ]
        mixed = jnp.concatenate(pieces, axis=0)
        cols = slice(g * group * conds, (g + 1) * group * conds)
        total[:, cols] += lax.dot_general(
            valence, mixed, (((1,), (1,)), ((), ())), preferred_element_type=jnp.float32
        )

    def finish(k):
        remote(k).wait()
        gap = level_cond_ref[k] - level_val_ref[k]
        coupling = kept[k] + landed[k].astype(jnp.float32)
        out_ref[k] = (gap * own_ref[k].astype(jnp.float32) + coupling).astype(out_ref.dtype)

    @pl.when(step == pl.num_programs(1) - 1)
    def _():
        away[at] = total[pl.ds(pl.multiple_of(other * val_rows, 8), val_rows), :].astype(away.dtype)
        remote(at).start()
        kept[at] = total[pl.ds(pl.multiple_of(me * val_rows, 8), val_rows), :]

        @pl.when(at >= 1)
        def _():
            finish(at - 1)

        @pl.when(at == kpoints - 1)
        def _():
            finish(at)


def backward_pair(image, orb_val, orb_cond, own, level_val, level_cond):
    kpoints, all_val, points_dev = orb_val.shape
    conds = orb_cond.shape[1]
    vectors = image.shape[0]
    val_rows, width = own.shape[1:]
    tile = pick_tile(points_dev, 1024)
    fixed = lambda k, i: (0, 0, 0)
    return pl.pallas_call(
        backward_pair_kernel,
        grid=(kpoints, points_dev // tile),
        out_shape=jax.ShapeDtypeStruct(own.shape, jnp.bfloat16),
        in_specs=[
            pl.BlockSpec((vectors, tile), lambda k, i: (0, i)),
            pl.BlockSpec((1, all_val, tile), lambda k, i: (k, 0, i)),
            pl.BlockSpec((1, conds, tile), lambda k, i: (k, 0, i)),
            pl.BlockSpec(own.shape, fixed),
            pl.BlockSpec(level_val.shape, fixed),
            pl.BlockSpec(level_cond.shape, fixed),
        ],
        out_specs=pl.BlockSpec(own.shape, fixed),
        scratch_shapes=[
            pltpu.VMEM((all_val, width), jnp.float32),
            pltpu.VMEM(own.shape, jnp.float32),
            pltpu.VMEM(own.shape, jnp.bfloat16),
            pltpu.VMEM(own.shape, jnp.bfloat16),
            pltpu.SemaphoreType.DMA((kpoints,)),
            pltpu.SemaphoreType.DMA((kpoints,)),
        ],
        compiler_params=pltpu.CompilerParams(
            vmem_limit_bytes=VMEM_BYTES, collective_id=2, has_side_effects=True
        ),
    )(image, orb_val, orb_cond, own, level_val, level_cond)


def body_direct(count, pairs, eps_val, eps_cond, orb_val, orb_cond, screened):
    val_rows, kpoints, width = pairs.shape
    conds = orb_cond.shape[1]
    vectors = width // conds
    own = jnp.transpose(pairs, (1, 0, 2))
    own_val = lax.dynamic_slice_in_dim(eps_val, lax.axis_index("pa") * val_rows, val_rows, 1)
    level_cond = jnp.tile(eps_cond, (1, vectors))[:, None, :]
    part = forward_pair(own, orb_val, orb_cond)
    image = middle(count, part, screened)
    result = backward_pair(image, orb_val, orb_cond, own, own_val[:, :, None], level_cond)
    return jnp.transpose(result, (1, 0, 2))


def body(count, planes, *args):
    pairs, orb_val, orb_cond, screened = args[0], args[3], args[4], args[5]
    points_dev, rows_dev = orb_val.shape[2], screened.shape[0]
    vectors = pairs.shape[2] // orb_cond.shape[1]
    aligned = points_dev % (128 * count) == 0 and rows_dev % 128 == 0 and points_dev % 256 == 0
    quarters = vectors // QUARTER
    even = vectors % (2 * QUARTER) == 0 and count % max(quarters, 1) == 0 and quarters % 2 == 0
    if planes == 2 and aligned and even and pairs.shape[0] % 16 == 0:
        return body_direct(count, *args)
    return body_plain(*args)


def solution(mesh):
    in_specs = (
        P("pa", "ka", None),
        P("ka", None),
        P("ka", None),
        P("ka", None, "pa"),
        P("ka", None, "pa"),
        P("ka", "pa"),
    )
    out_specs = P("pa", "ka", None)
    step = functools.partial(body, mesh.shape["ka"], mesh.shape["pa"])
    return jax.shard_map(step, mesh=mesh, in_specs=in_specs, out_specs=out_specs, check_vma=False)
```

```python
import functools

import jax
import jax.numpy as jnp
from jax import lax
from jax.experimental import pallas as pl
from jax.experimental.pallas import tpu as pltpu
from jax.sharding import PartitionSpec as P

VMEM_BYTES = 58 * 1024 * 1024


def pick_tile(extent, most):
    tile = most
    while extent % tile:
        tile //= 2
    return tile


def forward_kernel(vectors, pairs_ref, val_ref, cond_ref, out_ref, turned):
    kpoints, conds = cond_ref.shape[0], cond_ref.shape[1]
    tile = cond_ref.shape[2]

    @pl.when(pl.program_id(0) == 0)
    def _():
        for k in range(kpoints):
            turned[k] = pairs_ref[k].T

    group = 4
    wide = [cond_ref[k].astype(jnp.float32).reshape(conds // 8, 8, tile) for k in range(kpoints)]
    for g in range(vectors // group):
        total = None
        for k in range(kpoints):
            rows = turned[k, g * group * conds : (g + 1) * group * conds, :]
            inner = jnp.dot(rows, val_ref[k], preferred_element_type=jnp.float32)
            inner = inner.reshape(group, conds // 8, 8, tile)
            added = jnp.sum(inner * wide[k][None], axis=1)
            total = added if total is None else total + added
        out_ref[g * group : (g + 1) * group, :] = jnp.sum(total, axis=1)


def forward(rows, orb_val, orb_cond):
    kpoints, all_val, points_dev = orb_val.shape
    conds = orb_cond.shape[1]
    width = rows.shape[2]
    vectors = width // conds
    tile = pick_tile(points_dev, 256)
    return pl.pallas_call(
        functools.partial(forward_kernel, vectors),
        grid=(points_dev // tile,),
        out_shape=jax.ShapeDtypeStruct((vectors, points_dev), jnp.float32),
        in_specs=[
            pl.BlockSpec((kpoints, all_val, width), lambda i: (0, 0, 0)),
            pl.BlockSpec((kpoints, all_val, tile), lambda i: (0, 0, i)),
            pl.BlockSpec((kpoints, conds, tile), lambda i: (0, 0, i)),
        ],
        out_specs=pl.BlockSpec((vectors, tile), lambda i: (0, i)),
        scratch_shapes=[pltpu.VMEM((kpoints, width, all_val), jnp.bfloat16)],
        compiler_params=pltpu.CompilerParams(vmem_limit_bytes=VMEM_BYTES),
    )(rows, orb_val, orb_cond)


def backward_kernel(image_ref, val_ref, cond_ref, out_ref, total):
    vectors, tile = image_ref.shape
    conds = cond_ref.shape[1]
    group = 4
    step = pl.program_id(1)

    @pl.when(step == 0)
    def _():
        total[...] = jnp.zeros_like(total)

    valence = val_ref[0]
    conduction = cond_ref[0]
    for g in range(vectors // group):
        pieces = [
            jnp.broadcast_to(image_ref[b : b + 1, :], (conds, tile)) * conduction
            for b in range(g * group, (g + 1) * group)
        ]
        mixed = jnp.concatenate(pieces, axis=0)
        cols = slice(g * group * conds, (g + 1) * group * conds)
        total[:, cols] += lax.dot_general(
            valence, mixed, (((1,), (1,)), ((), ())), preferred_element_type=jnp.float32
        )

    @pl.when(step == pl.num_programs(1) - 1)
    def _():
        out_ref[0] = total[...].astype(out_ref.dtype)


def backward(image, orb_val, orb_cond):
    kpoints, all_val, points_dev = orb_val.shape
    conds = orb_cond.shape[1]
    vectors = image.shape[0]
    tile = pick_tile(points_dev, 1024)
    return pl.pallas_call(
        backward_kernel,
        grid=(kpoints, points_dev // tile),
        out_shape=jax.ShapeDtypeStruct((kpoints, all_val, vectors * conds), jnp.bfloat16),
        in_specs=[
            pl.BlockSpec((vectors, tile), lambda k, i: (0, i)),
            pl.BlockSpec((1, all_val, tile), lambda k, i: (k, 0, i)),
            pl.BlockSpec((1, conds, tile), lambda k, i: (k, 0, i)),
        ],
        out_specs=pl.BlockSpec((1, all_val, vectors * conds), lambda k, i: (k, 0, 0)),
        scratch_shapes=[pltpu.VMEM((all_val, vectors * conds), jnp.float32)],
        compiler_params=pltpu.CompilerParams(vmem_limit_bytes=VMEM_BYTES),
    )(image, orb_val, orb_cond)


def body_plain(pairs, eps_val, eps_cond, orb_val, orb_cond, screened):
    val_rows, kpoints, width = pairs.shape
    conds = orb_cond.shape[1]
    points_dev = orb_val.shape[2]
    vectors = width // conds
    own = jnp.transpose(pairs, (1, 0, 2))
    rows = lax.all_gather(own, "pa", axis=1, tiled=True)
    partial_points = forward(rows, orb_val, orb_cond)
    points = lax.psum_scatter(partial_points, "ka", scatter_dimension=1, tiled=True)
    points_bf = lax.all_gather(points.astype(jnp.bfloat16), "ka", axis=1, tiled=True)
    image_part = lax.dot_general(
        points_bf, screened, (((1,), (1,)), ((), ())), preferred_element_type=jnp.float32
    )
    image_rows = lax.psum(image_part.astype(jnp.bfloat16), "pa")
    image_whole = lax.all_gather(image_rows, "ka", axis=1, tiled=True)
    image_block = lax.dynamic_slice_in_dim(
        image_whole, lax.axis_index("pa") * points_dev, points_dev, 1
    )
    results = backward(image_block, orb_val, orb_cond)
    coupling = lax.psum_scatter(results, "pa", scatter_dimension=1, tiled=True)
    coupling = jnp.transpose(coupling.astype(jnp.float32), (1, 0, 2))
    own_val = lax.dynamic_slice_in_dim(eps_val, lax.axis_index("pa") * val_rows, val_rows, 1)
    energy_gap = eps_cond[None, :, None, :] - jnp.transpose(own_val)[:, :, None, None]
    coeffs = pairs.astype(jnp.float32).reshape(val_rows, kpoints, vectors, conds)
    diagonal_part = (energy_gap * coeffs).reshape(val_rows, kpoints, vectors * conds)
    return (diagonal_part + coupling).astype(jnp.bfloat16)


MESH = pl.DeviceIdType.MESH
QUARTER = 8


def front_kernel(
    count, own_ref, val_hbm, cond_hbm, screened_ref, out_ref, val_ref, cond_ref, near, full, turned, early,
    part_ref, landed, points, piece, summed, images, load_sem, pair_send, pair_recv,
    sum_send, sum_recv, pts_send, pts_recv, mix_send, mix_recv, img_send, img_recv,
):
    me, plane = lax.axis_index("ka"), lax.axis_index("pa")
    other = 1 - plane
    core = lax.rem(me, 2)
    partner = me + 1 - 2 * core
    share = landed.shape[2]
    kpoints, conds = cond_ref.shape[:2]
    rows_dev = near.shape[0]
    vectors, points_dev = points.shape
    tile = early.shape[2]
    quarters = vectors // QUARTER
    ring = count // quarters
    layers = quarters // 2
    chips = count // 2
    group = 4

    def cols(j, size):
        return pl.ds(pl.multiple_of(j * size, 128), size)

    loads = [
        pltpu.make_async_copy(own_ref, full.at[plane], load_sem.at[0]),
        pltpu.make_async_copy(val_hbm, val_ref, load_sem.at[1]),
        pltpu.make_async_copy(cond_hbm, cond_ref, load_sem.at[2]),
        pltpu.make_async_copy(screened_ref, near, load_sem.at[3]),
    ]
    for load in loads:
        load.start()

    barrier = pltpu.get_barrier_semaphore()
    for s in range(1, 2 * count):
        there = lax.rem(me * 2 + plane + s, 2 * count)
        pl.semaphore_signal(
            barrier, inc=1, device_id=(there // 2, lax.rem(there, 2)), device_id_type=MESH
        )
    pl.semaphore_wait(barrier, 2 * count - 1)

    def send_pairs(k):
        return pltpu.make_async_remote_copy(
            src_ref=own_ref.at[k],
            dst_ref=full.at[plane, k],
            send_sem=pair_send.at[k],
            recv_sem=pair_recv.at[k],
            device_id=(me, other),
            device_id_type=MESH,
        )

    def send_part(j, slot):
        return pltpu.make_async_remote_copy(
            src_ref=part_ref.at[:, cols(j, share)],
            dst_ref=landed.at[slot],
            send_sem=sum_send.at[j],
            recv_sem=sum_recv.at[slot],
            device_id=(j, plane),
            device_id_type=MESH,
        )

    def send_points(j, owner, slot):
        return pltpu.make_async_remote_copy(
            src_ref=points.at[:, cols(owner, share)],
            dst_ref=points.at[:, cols(owner, share)],
            send_sem=pts_send.at[slot],
            recv_sem=pts_recv.at[owner],
            device_id=(j, plane),
            device_id_type=MESH,
        )

    def send_images(j, owner, slot):
        return pltpu.make_async_remote_copy(
            src_ref=images.at[owner],
            dst_ref=images.at[owner],
            send_sem=img_send.at[slot],
            recv_sem=img_recv.at[owner],
            device_id=(j, plane),
            device_id_type=MESH,
        )

    def turn(k):
        send_pairs(k).wait()
        turned[k] = jnp.concatenate([full[0, k], full[1, k]], axis=0).T

    def contract(ks, g, at):
        total = None
        for k in ks:
            wide = cond_ref[k, :, at].astype(jnp.float32).reshape(conds // 8, 8, tile)
            rows = turned[k, g * group * conds : (g + 1) * group * conds, :]
            inner = jnp.dot(rows, val_ref[k, :, at], preferred_element_type=jnp.float32)
            inner = inner.reshape(group, conds // 8, 8, tile)
            added = jnp.sum(inner * wide[None], axis=1)
            total = added if total is None else total + added
        return jnp.sum(total, axis=1)

    for k in range(kpoints):
        send_pairs(k).start()
    for load in loads[:3]:
        load.wait()
    turn(0)

    def first(i, carry):
        for g in range(vectors // group):
            early[i, g * group : (g + 1) * group, :] = contract([0], g, cols(i, tile))
        return carry

    lax.fori_loop(0, points_dev // tile, first, 0)
    for k in range(1, kpoints):
        turn(k)

    pieces = 2 * share // tile

    def rest(s, carry):
        t = lax.rem(me // 2 + 1 + s, chips)

        def inner_tile(u, carry):
            i = t * pieces + u
            parts = [contract(range(1, kpoints), g, cols(i, tile)) for g in range(vectors // group)]
            part_ref[:, cols(i, tile)] = (jnp.concatenate(parts, axis=0) + early[i]).astype(
                jnp.bfloat16
            )
            return carry

        lax.fori_loop(0, pieces, inner_tile, 0)
        for e in range(2):
            j = t * 2 + e

            @pl.when(j != me)
            def _():
                send_part(j, me).start()

        return carry

    lax.fori_loop(0, chips, rest, 0)

    ahead = [lax.rem(me + s, count) for s in range(1, count)]
    behind = [lax.rem(me + count - s, count) for s in range(1, count)]
    same_ahead = [lax.rem(me + 2 * s, count) for s in range(1, chips)]
    same_behind = [lax.rem(me + count - 2 * s, count) for s in range(1, chips)]
    beside = [lax.rem(partner + count - 2 * s, count) for s in range(chips)]

    total = part_ref[:, cols(me, share)].astype(jnp.float32)
    for j in behind:
        send_part(j, j).wait_recv()
        total = total + landed[j].astype(jnp.float32)
    points[:, cols(me, share)] = total.astype(jnp.bfloat16)
    for j in same_ahead:
        send_points(j, me, j).start()
    send_points(partner, me, partner).start()
    for s, j in enumerate(same_behind):
        send_points(j, j, j).wait_recv()
        send_points(partner, j, count + s).start()

    loads[3].wait()
    image = None
    for j in beside:
        t = j // 2
        send_points(partner, j, partner).wait_recv()
        added = lax.dot_general(
            points[:, cols(t, 2 * share)],
            near[:, cols(t, 2 * share)],
            (((1,), (1,)), ((), ())),
            preferred_element_type=jnp.float32,
        )
        image = added if image is None else image + added
    for t in range(quarters):
        piece[t] = image[t * QUARTER : (t + 1) * QUARTER, :]

    z, r = me // ring, lax.rem(me, ring)
    target, layer = z // layers, lax.rem(z, layers)

    def send_piece(t, source_plane, source_layer):
        return pltpu.make_async_remote_copy(
            src_ref=piece.at[t],
            dst_ref=summed.at[source_plane, source_layer],
            send_sem=mix_send.at[t],
            recv_sem=mix_recv.at[source_plane * layers + source_layer],
            device_id=(t * ring + r, target),
            device_id_type=MESH,
        )

    for t in range(quarters):
        here = jnp.logical_and(target == plane, z == t)

        @pl.when(jnp.logical_not(here))
        def _():
            send_piece(t, plane, layer).start()

        @pl.when(here)
        def _():
            summed[plane, layer] = piece[t]

    for p in range(2):
        for h in range(layers):
            here = jnp.logical_and(p == plane, z == plane * layers + h)

            @pl.when(jnp.logical_not(here))
            def _():
                send_piece(0, p, h).wait_recv()

    for h in range(layers):
        images[me, :, h * rows_dev : (h + 1) * rows_dev] = (summed[0, h] + summed[1, h]).astype(
            jnp.bfloat16
        )
    for j in same_ahead:
        send_images(j, me, j).start()
    send_images(partner, me, partner).start()
    for s, j in enumerate(same_behind):
        send_images(j, j, j).wait_recv()
        send_images(partner, j, count + s).start()
    for j in ahead:
        send_part(j, me).wait_send()
    for j in same_ahead:
        send_points(j, me, j).wait_send()
    send_points(partner, me, partner).wait_send()
    for s, j in enumerate(same_behind):
        send_points(partner, j, count + s).wait_send()
    for t in range(quarters):
        here = jnp.logical_and(target == plane, z == t)

        @pl.when(jnp.logical_not(here))
        def _():
            send_piece(t, plane, layer).wait_send()

    for j in beside:
        send_images(partner, j, partner).wait_recv()
    for f in range(quarters // 2):
        for c in range(ring):
            both = jnp.concatenate(
                [images[(2 * f + e) * ring + c].astype(jnp.float32) for e in range(2)], axis=0
            ).astype(jnp.bfloat16)
            for h in range(layers):
                at = (h * ring + c) * rows_dev
                out_ref[f * 2 * QUARTER : (f + 1) * 2 * QUARTER, at : at + rows_dev] = both[
                    :, h * rows_dev : (h + 1) * rows_dev
                ]
    for j in same_ahead:
        send_images(j, me, j).wait_send()
    send_images(partner, me, partner).wait_send()
    for s, j in enumerate(same_behind):
        send_images(partner, j, count + s).wait_send()


def front(count, own, orb_val, orb_cond, screened):
    kpoints, all_val, points_dev = orb_val.shape
    conds = orb_cond.shape[1]
    val_rows, width = own.shape[1:]
    vectors = width // conds
    rows_dev = screened.shape[0]
    share = points_dev // count
    tile = 256
    quarters = vectors // QUARTER
    dma = pltpu.SemaphoreType.DMA
    return pl.pallas_call(
        functools.partial(front_kernel, count),
        out_shape=jax.ShapeDtypeStruct((vectors, points_dev), jnp.bfloat16),
        in_specs=[pl.BlockSpec(memory_space=pl.ANY)] * 4,
        out_specs=pl.BlockSpec(memory_space=pltpu.VMEM),
        scratch_shapes=[
            pltpu.VMEM(orb_val.shape, jnp.bfloat16),
            pltpu.VMEM(orb_cond.shape, jnp.bfloat16),
            pltpu.VMEM((rows_dev, points_dev), jnp.bfloat16),
            pltpu.VMEM((2, kpoints, val_rows, width), jnp.bfloat16),
            pltpu.VMEM((kpoints, width, all_val), jnp.bfloat16),
            pltpu.VMEM((points_dev // tile, vectors, tile), jnp.float32),
            pltpu.VMEM((vectors, points_dev), jnp.bfloat16),
            pltpu.VMEM((count, vectors, share), jnp.bfloat16),
            pltpu.VMEM((vectors, points_dev), jnp.bfloat16),
            pltpu.VMEM((quarters, QUARTER, rows_dev), jnp.float32),
            pltpu.VMEM((2, quarters // 2, QUARTER, rows_dev), jnp.float32),
            pltpu.VMEM((count, QUARTER, quarters // 2 * rows_dev), jnp.bfloat16),
            dma((4,)),
            dma((kpoints,)),
            dma((kpoints,)),
            dma((count,)),
            dma((count,)),
            dma((2 * count,)),
            dma((count,)),
            dma((quarters,)),
            dma((quarters,)),
            dma((2 * count,)),
            dma((count,)),
        ],
        compiler_params=pltpu.CompilerParams(
            vmem_limit_bytes=VMEM_BYTES, collective_id=0, has_side_effects=True
        ),
    )(own, orb_val, orb_cond, screened)


def backward_pair_kernel(
    image_ref, val_ref, cond_ref, own_ref, level_val_ref, level_cond_ref, out_ref,
    total, kept, away, landed, send_sem, recv_sem,
):
    vectors, tile = image_ref.shape
    conds = cond_ref.shape[1]
    kpoints, val_rows = own_ref.shape[:2]
    group = 4
    at, step = pl.program_id(0), pl.program_id(1)
    row, me = lax.axis_index("ka"), lax.axis_index("pa")
    other = 1 - me

    def remote(k):
        return pltpu.make_async_remote_copy(
            src_ref=away.at[k],
            dst_ref=landed.at[k],
            send_sem=send_sem.at[k],
            recv_sem=recv_sem.at[k],
            device_id=(row, other),
            device_id_type=MESH,
        )

    @pl.when(jnp.logical_and(at == 0, step == 0))
    def _():
        barrier = pltpu.get_barrier_semaphore()
        pl.semaphore_signal(barrier, inc=1, device_id=(row, other), device_id_type=MESH)
        pl.semaphore_wait(barrier, 1)

    @pl.when(step == 0)
    def _():
        total[...] = jnp.zeros_like(total)

    valence = val_ref[0]
    conduction = cond_ref[0]
    for g in range(vectors // group):
        pieces = [
            jnp.broadcast_to(image_ref[b : b + 1, :], (conds, tile)) * conduction
            for b in range(g * group, (g + 1) * group)
        ]
        mixed = jnp.concatenate(pieces, axis=0)
        cols = slice(g * group * conds, (g + 1) * group * conds)
        total[:, cols] += lax.dot_general(
            valence, mixed, (((1,), (1,)), ((), ())), preferred_element_type=jnp.float32
        )

    def finish(k):
        remote(k).wait()
        gap = level_cond_ref[k] - level_val_ref[k]
        coupling = kept[k] + landed[k].astype(jnp.float32)
        out_ref[k] = (gap * own_ref[k].astype(jnp.float32) + coupling).astype(out_ref.dtype)

    @pl.when(step == pl.num_programs(1) - 1)
    def _():
        away[at] = total[pl.ds(pl.multiple_of(other * val_rows, 8), val_rows), :].astype(away.dtype)
        remote(at).start()
        kept[at] = total[pl.ds(pl.multiple_of(me * val_rows, 8), val_rows), :]

        @pl.when(at >= 1)
        def _():
            finish(at - 1)

        @pl.when(at == kpoints - 1)
        def _():
            finish(at)


def backward_pair(image, orb_val, orb_cond, own, level_val, level_cond):
    kpoints, all_val, points_dev = orb_val.shape
    conds = orb_cond.shape[1]
    vectors = image.shape[0]
    val_rows, width = own.shape[1:]
    tile = pick_tile(points_dev, 2048)
    fixed = lambda k, i: (0, 0, 0)
    return pl.pallas_call(
        backward_pair_kernel,
        grid=(kpoints, points_dev // tile),
        out_shape=jax.ShapeDtypeStruct(own.shape, jnp.bfloat16),
        in_specs=[
            pl.BlockSpec((vectors, tile), lambda k, i: (0, i)),
            pl.BlockSpec((1, all_val, tile), lambda k, i: (k, 0, i)),
            pl.BlockSpec((1, conds, tile), lambda k, i: (k, 0, i)),
            pl.BlockSpec(own.shape, fixed),
            pl.BlockSpec(level_val.shape, fixed),
            pl.BlockSpec(level_cond.shape, fixed),
        ],
        out_specs=pl.BlockSpec(own.shape, fixed),
        scratch_shapes=[
            pltpu.VMEM((all_val, width), jnp.float32),
            pltpu.VMEM(own.shape, jnp.float32),
            pltpu.VMEM(own.shape, jnp.bfloat16),
            pltpu.VMEM(own.shape, jnp.bfloat16),
            pltpu.SemaphoreType.DMA((kpoints,)),
            pltpu.SemaphoreType.DMA((kpoints,)),
        ],
        compiler_params=pltpu.CompilerParams(
            vmem_limit_bytes=VMEM_BYTES, collective_id=1, has_side_effects=True
        ),
    )(image, orb_val, orb_cond, own, level_val, level_cond)


def body_direct(count, pairs, eps_val, eps_cond, orb_val, orb_cond, screened):
    val_rows, kpoints, width = pairs.shape
    conds = orb_cond.shape[1]
    vectors = width // conds
    own = jnp.transpose(pairs, (1, 0, 2))
    own_val = lax.dynamic_slice_in_dim(eps_val, lax.axis_index("pa") * val_rows, val_rows, 1)
    level_cond = jnp.tile(eps_cond, (1, vectors))[:, None, :]
    image = front(count, own, orb_val, orb_cond, screened)
    result = backward_pair(image, orb_val, orb_cond, own, own_val[:, :, None], level_cond)
    return jnp.transpose(result, (1, 0, 2))


def body(count, planes, *args):
    pairs, orb_val, orb_cond, screened = args[0], args[3], args[4], args[5]
    points_dev, rows_dev = orb_val.shape[2], screened.shape[0]
    vectors = pairs.shape[2] // orb_cond.shape[1]
    aligned = points_dev % (128 * count) == 0 and rows_dev % 128 == 0 and points_dev % (256 * count // 2) == 0
    quarters = vectors // QUARTER
    even = vectors % (2 * QUARTER) == 0 and count % max(quarters, 1) == 0 and quarters % 2 == 0
    if planes == 2 and aligned and even and pairs.shape[0] % 16 == 0:
        return body_direct(count, *args)
    return body_plain(*args)


def solution(mesh):
    in_specs = (
        P("pa", "ka", None),
        P("ka", None),
        P("ka", None),
        P("ka", None, "pa"),
        P("ka", None, "pa"),
        P("ka", "pa"),
    )
    out_specs = P("pa", "ka", None)
    step = functools.partial(body, mesh.shape["ka"], mesh.shape["pa"])
    return jax.shard_map(step, mesh=mesh, in_specs=in_specs, out_specs=out_specs, check_vma=False)
```

```python
import functools

import jax
import jax.numpy as jnp
from jax import lax
from jax.experimental import pallas as pl
from jax.experimental.pallas import tpu as pltpu
from jax.sharding import PartitionSpec as P

VMEM_BYTES = 58 * 1024 * 1024


def pick_tile(extent, most):
    tile = most
    while extent % tile:
        tile //= 2
    return tile


def forward_kernel(vectors, pairs_ref, val_ref, cond_ref, out_ref, turned):
    kpoints, conds = cond_ref.shape[0], cond_ref.shape[1]
    tile = cond_ref.shape[2]

    @pl.when(pl.program_id(0) == 0)
    def _():
        for k in range(kpoints):
            turned[k] = pairs_ref[k].T

    group = 4
    wide = [cond_ref[k].astype(jnp.float32).reshape(conds // 8, 8, tile) for k in range(kpoints)]
    for g in range(vectors // group):
        total = None
        for k in range(kpoints):
            rows = turned[k, g * group * conds : (g + 1) * group * conds, :]
            inner = jnp.dot(rows, val_ref[k], preferred_element_type=jnp.float32)
            inner = inner.reshape(group, conds // 8, 8, tile)
            added = jnp.sum(inner * wide[k][None], axis=1)
            total = added if total is None else total + added
        out_ref[g * group : (g + 1) * group, :] = jnp.sum(total, axis=1)


def forward(rows, orb_val, orb_cond):
    kpoints, all_val, points_dev = orb_val.shape
    conds = orb_cond.shape[1]
    width = rows.shape[2]
    vectors = width // conds
    tile = pick_tile(points_dev, 256)
    return pl.pallas_call(
        functools.partial(forward_kernel, vectors),
        grid=(points_dev // tile,),
        out_shape=jax.ShapeDtypeStruct((vectors, points_dev), jnp.float32),
        in_specs=[
            pl.BlockSpec((kpoints, all_val, width), lambda i: (0, 0, 0)),
            pl.BlockSpec((kpoints, all_val, tile), lambda i: (0, 0, i)),
            pl.BlockSpec((kpoints, conds, tile), lambda i: (0, 0, i)),
        ],
        out_specs=pl.BlockSpec((vectors, tile), lambda i: (0, i)),
        scratch_shapes=[pltpu.VMEM((kpoints, width, all_val), jnp.bfloat16)],
        compiler_params=pltpu.CompilerParams(vmem_limit_bytes=VMEM_BYTES),
    )(rows, orb_val, orb_cond)


def backward_kernel(image_ref, val_ref, cond_ref, out_ref, total):
    vectors, tile = image_ref.shape
    conds = cond_ref.shape[1]
    group = 4
    step = pl.program_id(1)

    @pl.when(step == 0)
    def _():
        total[...] = jnp.zeros_like(total)

    valence = val_ref[0]
    conduction = cond_ref[0]
    for g in range(vectors // group):
        pieces = [
            jnp.broadcast_to(image_ref[b : b + 1, :], (conds, tile)) * conduction
            for b in range(g * group, (g + 1) * group)
        ]
        mixed = jnp.concatenate(pieces, axis=0)
        cols = slice(g * group * conds, (g + 1) * group * conds)
        total[:, cols] += lax.dot_general(
            valence, mixed, (((1,), (1,)), ((), ())), preferred_element_type=jnp.float32
        )

    @pl.when(step == pl.num_programs(1) - 1)
    def _():
        out_ref[0] = total[...].astype(out_ref.dtype)


def backward(image, orb_val, orb_cond):
    kpoints, all_val, points_dev = orb_val.shape
    conds = orb_cond.shape[1]
    vectors = image.shape[0]
    tile = pick_tile(points_dev, 1024)
    return pl.pallas_call(
        backward_kernel,
        grid=(kpoints, points_dev // tile),
        out_shape=jax.ShapeDtypeStruct((kpoints, all_val, vectors * conds), jnp.bfloat16),
        in_specs=[
            pl.BlockSpec((vectors, tile), lambda k, i: (0, i)),
            pl.BlockSpec((1, all_val, tile), lambda k, i: (k, 0, i)),
            pl.BlockSpec((1, conds, tile), lambda k, i: (k, 0, i)),
        ],
        out_specs=pl.BlockSpec((1, all_val, vectors * conds), lambda k, i: (k, 0, 0)),
        scratch_shapes=[pltpu.VMEM((all_val, vectors * conds), jnp.float32)],
        compiler_params=pltpu.CompilerParams(vmem_limit_bytes=VMEM_BYTES),
    )(image, orb_val, orb_cond)


def body_plain(pairs, eps_val, eps_cond, orb_val, orb_cond, screened):
    val_rows, kpoints, width = pairs.shape
    conds = orb_cond.shape[1]
    points_dev = orb_val.shape[2]
    vectors = width // conds
    own = jnp.transpose(pairs, (1, 0, 2))
    rows = lax.all_gather(own, "pa", axis=1, tiled=True)
    partial_points = forward(rows, orb_val, orb_cond)
    points = lax.psum_scatter(partial_points, "ka", scatter_dimension=1, tiled=True)
    points_bf = lax.all_gather(points.astype(jnp.bfloat16), "ka", axis=1, tiled=True)
    image_part = lax.dot_general(
        points_bf, screened, (((1,), (1,)), ((), ())), preferred_element_type=jnp.float32
    )
    image_rows = lax.psum(image_part.astype(jnp.bfloat16), "pa")
    image_whole = lax.all_gather(image_rows, "ka", axis=1, tiled=True)
    image_block = lax.dynamic_slice_in_dim(
        image_whole, lax.axis_index("pa") * points_dev, points_dev, 1
    )
    results = backward(image_block, orb_val, orb_cond)
    coupling = lax.psum_scatter(results, "pa", scatter_dimension=1, tiled=True)
    coupling = jnp.transpose(coupling.astype(jnp.float32), (1, 0, 2))
    own_val = lax.dynamic_slice_in_dim(eps_val, lax.axis_index("pa") * val_rows, val_rows, 1)
    energy_gap = eps_cond[None, :, None, :] - jnp.transpose(own_val)[:, :, None, None]
    coeffs = pairs.astype(jnp.float32).reshape(val_rows, kpoints, vectors, conds)
    diagonal_part = (energy_gap * coeffs).reshape(val_rows, kpoints, vectors * conds)
    return (diagonal_part + coupling).astype(jnp.bfloat16)


MESH = pl.DeviceIdType.MESH
QUARTER = 8


def front_kernel(
    count, own_ref, val_hbm, cond_hbm, screened_ref, out_ref, val_ref, cond_ref, near, full, turned, early,
    part_ref, landed, points, piece, summed, images, load_sem, pair_send, pair_recv,
    sum_send, sum_recv, pts_send, pts_recv, mix_send, mix_recv, img_send, img_recv,
):
    me, plane = lax.axis_index("ka"), lax.axis_index("pa")
    other = 1 - plane
    core = lax.rem(me, 2)
    partner = me + 1 - 2 * core
    share = landed.shape[2]
    kpoints, conds = cond_ref.shape[:2]
    rows_dev = near.shape[0]
    vectors, points_dev = points.shape
    tile = early.shape[2]
    quarters = vectors // QUARTER
    ring = count // quarters
    layers = quarters // 2
    chips = count // 2
    group = 4

    def cols(j, size):
        return pl.ds(pl.multiple_of(j * size, 128), size)

    loads = [
        pltpu.make_async_copy(own_ref, full.at[plane], load_sem.at[0]),
        pltpu.make_async_copy(val_hbm, val_ref, load_sem.at[1]),
        pltpu.make_async_copy(cond_hbm, cond_ref, load_sem.at[2]),
        pltpu.make_async_copy(screened_ref, near, load_sem.at[3]),
    ]
    for load in loads:
        load.start()

    barrier = pltpu.get_barrier_semaphore()
    for s in range(1, 2 * count):
        there = lax.rem(me * 2 + plane + s, 2 * count)
        pl.semaphore_signal(
            barrier, inc=1, device_id=(there // 2, lax.rem(there, 2)), device_id_type=MESH
        )
    pl.semaphore_wait(barrier, 2 * count - 1)

    def send_pairs(k):
        return pltpu.make_async_remote_copy(
            src_ref=own_ref.at[k],
            dst_ref=full.at[plane, k],
            send_sem=pair_send.at[k],
            recv_sem=pair_recv.at[k],
            device_id=(me, other),
            device_id_type=MESH,
        )

    def send_part(j, slot):
        return pltpu.make_async_remote_copy(
            src_ref=part_ref.at[:, cols(j, share)],
            dst_ref=landed.at[slot],
            send_sem=sum_send.at[j],
            recv_sem=sum_recv.at[slot],
            device_id=(j, plane),
            device_id_type=MESH,
        )

    def send_points(j, owner, slot):
        return pltpu.make_async_remote_copy(
            src_ref=points.at[:, cols(owner, share)],
            dst_ref=points.at[:, cols(owner, share)],
            send_sem=pts_send.at[slot],
            recv_sem=pts_recv.at[owner],
            device_id=(j, plane),
            device_id_type=MESH,
        )

    def send_images(j, owner, slot):
        return pltpu.make_async_remote_copy(
            src_ref=images.at[owner],
            dst_ref=images.at[owner],
            send_sem=img_send.at[slot],
            recv_sem=img_recv.at[owner],
            device_id=(j, plane),
            device_id_type=MESH,
        )

    def turn(k):
        send_pairs(k).wait()
        turned[k] = jnp.concatenate([full[0, k], full[1, k]], axis=0).T

    def contract(ks, g, at):
        total = None
        for k in ks:
            wide = cond_ref[k, :, at].astype(jnp.float32).reshape(conds // 8, 8, tile)
            rows = turned[k, g * group * conds : (g + 1) * group * conds, :]
            inner = jnp.dot(rows, val_ref[k, :, at], preferred_element_type=jnp.float32)
            inner = inner.reshape(group, conds // 8, 8, tile)
            added = jnp.sum(inner * wide[None], axis=1)
            total = added if total is None else total + added
        return jnp.sum(total, axis=1)

    for k in range(kpoints):
        send_pairs(k).start()
    for load in loads[:3]:
        load.wait()
    turn(0)

    def first(i, carry):
        for g in range(vectors // group):
            early[i, g * group : (g + 1) * group, :] = contract([0], g, cols(i, tile))
        return carry

    lax.fori_loop(0, points_dev // tile, first, 0)
    for k in range(1, kpoints):
        turn(k)

    pieces = 2 * share // tile

    def rest(s, carry):
        t = lax.rem(me // 2 + 1 + s, chips)

        def inner_tile(u, carry):
            i = t * pieces + u
            parts = [contract(range(1, kpoints), g, cols(i, tile)) for g in range(vectors // group)]
            part_ref[:, cols(i, tile)] = (jnp.concatenate(parts, axis=0) + early[i]).astype(
                jnp.bfloat16
            )
            return carry

        lax.fori_loop(0, pieces, inner_tile, 0)
        for e in range(2):
            j = t * 2 + e

            @pl.when(j != me)
            def _():
                send_part(j, me).start()

        return carry

    lax.fori_loop(0, chips, rest, 0)

    ahead = [lax.rem(me + s, count) for s in range(1, count)]
    behind = [lax.rem(me + count - s, count) for s in range(1, count)]
    same_ahead = [lax.rem(me + 2 * s, count) for s in range(1, chips)]
    same_behind = [lax.rem(me + count - 2 * s, count) for s in range(1, chips)]
    beside = [lax.rem(partner + count - 2 * s, count) for s in range(chips)]

    total = part_ref[:, cols(me, share)].astype(jnp.float32)
    for j in behind:
        send_part(j, j).wait_recv()
        total = total + landed[j].astype(jnp.float32)
    points[:, cols(me, share)] = total.astype(jnp.bfloat16)
    for j in same_ahead:
        send_points(j, me, j).start()
    send_points(partner, me, partner).start()
    for s, j in enumerate(same_behind):
        send_points(j, j, j).wait_recv()
        send_points(partner, j, count + s).start()

    loads[3].wait()
    image = None
    for j in beside:
        t = j // 2
        send_points(partner, j, partner).wait_recv()
        added = lax.dot_general(
            points[:, cols(t, 2 * share)],
            near[:, cols(t, 2 * share)],
            (((1,), (1,)), ((), ())),
            preferred_element_type=jnp.float32,
        )
        image = added if image is None else image + added
    for t in range(quarters):
        piece[t] = image[t * QUARTER : (t + 1) * QUARTER, :]

    z, r = me // ring, lax.rem(me, ring)
    target, layer = z // layers, lax.rem(z, layers)

    def send_piece(t, source_plane, source_layer):
        return pltpu.make_async_remote_copy(
            src_ref=piece.at[t],
            dst_ref=summed.at[source_plane, source_layer],
            send_sem=mix_send.at[t],
            recv_sem=mix_recv.at[source_plane * layers + source_layer],
            device_id=(t * ring + r, target),
            device_id_type=MESH,
        )

    for t in range(quarters):
        here = jnp.logical_and(target == plane, z == t)

        @pl.when(jnp.logical_not(here))
        def _():
            send_piece(t, plane, layer).start()

        @pl.when(here)
        def _():
            summed[plane, layer] = piece[t]

    for p in range(2):
        for h in range(layers):
            here = jnp.logical_and(p == plane, z == plane * layers + h)

            @pl.when(jnp.logical_not(here))
            def _():
                send_piece(0, p, h).wait_recv()

    for h in range(layers):
        images[me, :, h * rows_dev : (h + 1) * rows_dev] = (summed[0, h] + summed[1, h]).astype(
            jnp.bfloat16
        )
    for j in same_ahead:
        send_images(j, me, j).start()
    send_images(partner, me, partner).start()
    for s, j in enumerate(same_behind):
        send_images(j, j, j).wait_recv()
        send_images(partner, j, count + s).start()
    for j in ahead:
        send_part(j, me).wait_send()
    for j in same_ahead:
        send_points(j, me, j).wait_send()
    send_points(partner, me, partner).wait_send()
    for s, j in enumerate(same_behind):
        send_points(partner, j, count + s).wait_send()
    for t in range(quarters):
        here = jnp.logical_and(target == plane, z == t)

        @pl.when(jnp.logical_not(here))
        def _():
            send_piece(t, plane, layer).wait_send()

    for j in beside:
        send_images(partner, j, partner).wait_recv()
    for f in range(quarters // 2):
        for c in range(ring):
            both = jnp.concatenate(
                [images[(2 * f + e) * ring + c].astype(jnp.float32) for e in range(2)], axis=0
            ).astype(jnp.bfloat16)
            for h in range(layers):
                at = (h * ring + c) * rows_dev
                out_ref[f * 2 * QUARTER : (f + 1) * 2 * QUARTER, at : at + rows_dev] = both[
                    :, h * rows_dev : (h + 1) * rows_dev
                ]
    for j in same_ahead:
        send_images(j, me, j).wait_send()
    send_images(partner, me, partner).wait_send()
    for s, j in enumerate(same_behind):
        send_images(partner, j, count + s).wait_send()


def front(count, own, orb_val, orb_cond, screened):
    kpoints, all_val, points_dev = orb_val.shape
    conds = orb_cond.shape[1]
    val_rows, width = own.shape[1:]
    vectors = width // conds
    rows_dev = screened.shape[0]
    share = points_dev // count
    tile = 256
    quarters = vectors // QUARTER
    dma = pltpu.SemaphoreType.DMA
    return pl.pallas_call(
        functools.partial(front_kernel, count),
        out_shape=jax.ShapeDtypeStruct((vectors, points_dev), jnp.bfloat16),
        in_specs=[pl.BlockSpec(memory_space=pl.ANY)] * 4,
        out_specs=pl.BlockSpec(memory_space=pltpu.VMEM),
        scratch_shapes=[
            pltpu.VMEM(orb_val.shape, jnp.bfloat16),
            pltpu.VMEM(orb_cond.shape, jnp.bfloat16),
            pltpu.VMEM((rows_dev, points_dev), jnp.bfloat16),
            pltpu.VMEM((2, kpoints, val_rows, width), jnp.bfloat16),
            pltpu.VMEM((kpoints, width, all_val), jnp.bfloat16),
            pltpu.VMEM((points_dev // tile, vectors, tile), jnp.float32),
            pltpu.VMEM((vectors, points_dev), jnp.bfloat16),
            pltpu.VMEM((count, vectors, share), jnp.bfloat16),
            pltpu.VMEM((vectors, points_dev), jnp.bfloat16),
            pltpu.VMEM((quarters, QUARTER, rows_dev), jnp.float32),
            pltpu.VMEM((2, quarters // 2, QUARTER, rows_dev), jnp.float32),
            pltpu.VMEM((count, QUARTER, quarters // 2 * rows_dev), jnp.bfloat16),
            dma((4,)),
            dma((kpoints,)),
            dma((kpoints,)),
            dma((count,)),
            dma((count,)),
            dma((2 * count,)),
            dma((count,)),
            dma((quarters,)),
            dma((quarters,)),
            dma((2 * count,)),
            dma((count,)),
        ],
        compiler_params=pltpu.CompilerParams(
            vmem_limit_bytes=VMEM_BYTES, collective_id=0, has_side_effects=True
        ),
    )(own, orb_val, orb_cond, screened)


def backward_pair_kernel(
    image_ref, val_ref, cond_ref, own_ref, level_val_ref, level_cond_ref, out_ref,
    total, streamed, kept, away, landed, send_sem, recv_sem,
):
    vectors, tile = image_ref.shape
    conds = cond_ref.shape[1]
    kpoints, val_rows = own_ref.shape[:2]
    group = 4
    at, step = pl.program_id(0), pl.program_id(1)
    row, me = lax.axis_index("ka"), lax.axis_index("pa")
    other = 1 - me

    def remote(k):
        return pltpu.make_async_remote_copy(
            src_ref=away.at[k],
            dst_ref=landed.at[k],
            send_sem=send_sem.at[k],
            recv_sem=recv_sem.at[k],
            device_id=(row, other),
            device_id_type=MESH,
        )

    @pl.when(jnp.logical_and(at == 0, step == 0))
    def _():
        barrier = pltpu.get_barrier_semaphore()
        pl.semaphore_signal(barrier, inc=1, device_id=(row, other), device_id_type=MESH)
        pl.semaphore_wait(barrier, 1)

    @pl.when(step == 0)
    def _():
        total[...] = jnp.zeros_like(total)
        streamed[...] = jnp.zeros_like(streamed)

    valence = val_ref[0]
    conduction = cond_ref[0]
    half = vectors // 2

    def products(start, stop):
        pieces = [
            jnp.broadcast_to(image_ref[b : b + 1, :], (conds, tile)) * conduction
            for b in range(start, stop)
        ]
        return jnp.concatenate(pieces, axis=0)

    streamed[...] += lax.dot_general(
        products(half, vectors),
        valence,
        (((1,), (1,)), ((), ())),
        preferred_element_type=jnp.float32,
    )
    for g in range(half // group):
        cols = slice(g * group * conds, (g + 1) * group * conds)
        total[:, cols] += lax.dot_general(
            valence,
            products(g * group, (g + 1) * group),
            (((1,), (1,)), ((), ())),
            preferred_element_type=jnp.float32,
        )

    def finish(k):
        remote(k).wait()
        gap = level_cond_ref[k] - level_val_ref[k]
        coupling = kept[k] + landed[k].astype(jnp.float32)
        out_ref[k] = (gap * own_ref[k].astype(jnp.float32) + coupling).astype(out_ref.dtype)

    @pl.when(step == pl.num_programs(1) - 1)
    def _():
        total[:, half * conds :] = streamed[...].T
        away[at] = total[pl.ds(pl.multiple_of(other * val_rows, 8), val_rows), :].astype(away.dtype)
        remote(at).start()
        kept[at] = total[pl.ds(pl.multiple_of(me * val_rows, 8), val_rows), :]

        @pl.when(at >= 1)
        def _():
            finish(at - 1)

        @pl.when(at == kpoints - 1)
        def _():
            finish(at)


def backward_pair(image, orb_val, orb_cond, own, level_val, level_cond):
    kpoints, all_val, points_dev = orb_val.shape
    conds = orb_cond.shape[1]
    vectors = image.shape[0]
    val_rows, width = own.shape[1:]
    tile = pick_tile(points_dev, 1024)
    fixed = lambda k, i: (0, 0, 0)
    return pl.pallas_call(
        backward_pair_kernel,
        grid=(kpoints, points_dev // tile),
        out_shape=jax.ShapeDtypeStruct(own.shape, jnp.bfloat16),
        in_specs=[
            pl.BlockSpec((vectors, tile), lambda k, i: (0, i)),
            pl.BlockSpec((1, all_val, tile), lambda k, i: (k, 0, i)),
            pl.BlockSpec((1, conds, tile), lambda k, i: (k, 0, i)),
            pl.BlockSpec(own.shape, fixed),
            pl.BlockSpec(level_val.shape, fixed),
            pl.BlockSpec(level_cond.shape, fixed),
        ],
        out_specs=pl.BlockSpec(own.shape, fixed),
        scratch_shapes=[
            pltpu.VMEM((all_val, width), jnp.float32),
            pltpu.VMEM((width // 2, all_val), jnp.float32),
            pltpu.VMEM(own.shape, jnp.float32),
            pltpu.VMEM(own.shape, jnp.bfloat16),
            pltpu.VMEM(own.shape, jnp.bfloat16),
            pltpu.SemaphoreType.DMA((kpoints,)),
            pltpu.SemaphoreType.DMA((kpoints,)),
        ],
        compiler_params=pltpu.CompilerParams(
            vmem_limit_bytes=VMEM_BYTES, collective_id=1, has_side_effects=True
        ),
    )(image, orb_val, orb_cond, own, level_val, level_cond)


def body_direct(count, pairs, eps_val, eps_cond, orb_val, orb_cond, screened):
    val_rows, kpoints, width = pairs.shape
    conds = orb_cond.shape[1]
    vectors = width // conds
    own = jnp.transpose(pairs, (1, 0, 2))
    own_val = lax.dynamic_slice_in_dim(eps_val, lax.axis_index("pa") * val_rows, val_rows, 1)
    level_cond = jnp.tile(eps_cond, (1, vectors))[:, None, :]
    image = front(count, own, orb_val, orb_cond, screened)
    result = backward_pair(image, orb_val, orb_cond, own, own_val[:, :, None], level_cond)
    return jnp.transpose(result, (1, 0, 2))


def body(count, planes, *args):
    pairs, orb_val, orb_cond, screened = args[0], args[3], args[4], args[5]
    points_dev, rows_dev = orb_val.shape[2], screened.shape[0]
    vectors = pairs.shape[2] // orb_cond.shape[1]
    aligned = points_dev % (128 * count) == 0 and rows_dev % 128 == 0 and points_dev % (256 * count // 2) == 0
    quarters = vectors // QUARTER
    even = vectors % (2 * QUARTER) == 0 and count % max(quarters, 1) == 0 and quarters % 2 == 0
    if planes == 2 and aligned and even and pairs.shape[0] % 16 == 0:
        return body_direct(count, *args)
    return body_plain(*args)


def solution(mesh):
    in_specs = (
        P("pa", "ka", None),
        P("ka", None),
        P("ka", None),
        P("ka", None, "pa"),
        P("ka", None, "pa"),
        P("ka", "pa"),
    )
    out_specs = P("pa", "ka", None)
    step = functools.partial(body, mesh.shape["ka"], mesh.shape["pa"])
    return jax.shard_map(step, mesh=mesh, in_specs=in_specs, out_specs=out_specs, check_vma=False)
```
